256 devices in a mesh: prow: 32 (over y, z_hi, core), pcol: 8 (over x, z_lo).
Axes of the slice: x: 4, y: 4, z: 8 (z_hi: 4, z_lo: 2; z = z_hi * 2 + z_lo), core: 2. Of those that a mesh axis runs over, the one named last changes fastest.
Arguments:
- factor_panel: float32 [2048, 63488], P('pcol', 'prow'), may hold values from -0.0234375 to 0.0234375
- whitened_before: float32 [63488, 4096], P('prow', 'pcol'), may hold values from -6 to 6
- green_panel: float32 [2048, 4096], P('prow', 'pcol'), may hold values from -6 to 6
- diag_inverse: float32 [2048, 2048], P('prow', 'pcol'), may hold values from -1 to 8, as said below
Outputs:
- whitened: float32 [2048, 4096], P('prow', 'pcol')
- gram_block: float32 [4096, 4096], P('prow', 'pcol')
The draws below stay inside these ranges and needn't reach their ends.
Inputs may be any that keep to these rules, and one draw needn't show every extreme that they name: `diag_inverse`: zero above the diagonal and positive on it.
All inputs are finite; a program needn't handle non-finite values.
Results may differ from the reference program's by a relative error of at most 0.00012.
Values sent between devices are 32-bit elements; how exact they have to be, the bound alone decides.
A program may use at most 128 MiB of HBM per device.

```python
import math
import jax
import jax.numpy as jnp
from jax import lax

P_SIZE = 4096
B = 2048
K = 63488


def draw_diag_inverse(key, part):
    first_key, second_key = jax.random.split(jax.random.fold_in(key, 7), 2)
    lower = jax.random.normal(first_key, (B, B), jnp.float32) * (0.7 / math.sqrt(B))
    diagonal = jnp.exp(jax.random.uniform(second_key, (B,), jnp.float32, math.log(0.5), math.log(2.0)))
    matrix = jnp.tril(lower, -1) + jnp.diag(diagonal)
    return matrix


def block_scale(rng, dims, cuts, low, high):
    def one(position, shards_of):
        steps = jax.random.uniform(jax.random.fold_in(jax.random.fold_in(rng, 6), position), (shards_of,), jnp.float32, low / len(cuts), high / len(cuts))
        return jnp.repeat(jnp.exp(steps), dims[position] // shards_of).reshape((-1,) + (1,) * (len(dims) - position - 1))

    gain = one(*cuts[0])
    for cut in cuts[1:]:
        gain = gain * one(*cut)
    return gain


def scatter_about(own_key, extent, spread, reach, pieces=(), dtype=jnp.bfloat16):
    entries = spread * jax.random.normal(own_key, extent, jnp.float32)
    if pieces:
        entries = entries * block_scale(own_key, extent, pieces, -0.22, 0.18)
    return jnp.clip(entries, -reach, reach).astype(dtype)


def setup_inputs(seed: int = 0) -> dict:
    streams_of = jax.random.split(jax.random.key(seed), 5)
    factor_panel = scatter_about(streams_of[0], (B, K), K ** -0.5, 0.0234375, ((0, 8), (1, 32)), jnp.float32)
    whitened_before = scatter_about(streams_of[1], (K, P_SIZE), 1.0, 6.0, ((0, 32), (1, 8)), jnp.float32)
    green_panel = scatter_about(streams_of[2], (B, P_SIZE), 1.0, 6.0, ((0, 32), (1, 8)), jnp.float32)
    diag_inverse = draw_diag_inverse(jax.random.fold_in(streams_of[4], 71), 0)
    return {"factor_panel": factor_panel, "whitened_before": whitened_before, "green_panel": green_panel, "diag_inverse": diag_inverse}


def reference(factor_panel, whitened_before, green_panel, diag_inverse):
    highest = lax.Precision.HIGHEST
    remaining = green_panel - jnp.dot(factor_panel, whitened_before, precision=highest, preferred_element_type=jnp.float32)
    whitened = jnp.dot(diag_inverse, remaining, precision=highest, preferred_element_type=jnp.float32)
    gram_block = jnp.dot(whitened.T, whitened, precision=highest, preferred_element_type=jnp.float32) * (1.0 / B)
    return whitened, gram_block
```

```python
import jax
import jax.numpy as jnp
from jax import lax
from jax.experimental import pallas as pl
from jax.experimental.pallas import tpu as pltpu
from jax.sharding import PartitionSpec as P

F32 = jnp.float32
BF16 = jnp.bfloat16
MESH = pl.DeviceIdType.MESH
ROWS = 2048
KD = 1984
KP = 2048
NSEM = 96


def split(v):
    hi = v.astype(BF16)
    return hi, (v - hi.astype(F32)).astype(BF16)


def mm(a, b, dims):
    return lax.dot_general(a, b, (dims, ((), ())), preferred_element_type=F32)


def mm3(ah, al, bh, bl, dims):
    return mm(ah, bh, dims) + (mm(ah, bl, dims) + mm(al, bh, dims))


def kernel(ft, wb, g, di, w_out, gram_out, FT, FTh, FTl, WB, WTh, WTl, PT, RC, RY1, RY2,
           RZ1, RZ2, RG, DS, DSh, WA, LB, ssem, rsem, lsem):
    r = lax.axis_index("prow")
    c = lax.axis_index("pcol")
    core = r % 2
    z0, z1 = (r // 2) % 2, (r // 4) % 2
    y0, y1 = (r // 8) % 2, r // 16
    zl = c % 2
    x0, x1 = (c // 2) % 2, c // 4
    zh, y, x = z0 + 2 * z1, y0 + 2 * y1, x0 + 2 * x1

    def near(b0, b1, base, unit):
        p1 = base + unit * (1 - 2 * b0)
        return p1, p1 + 2 * unit * (1 - 2 * b1), base + 2 * unit * (1 - 2 * b1)

    r_core = r + 1 - 2 * core
    r_z1, r_z3, _ = near(z0, z1, r, 2)
    r_y1, r_y3, _ = near(y0, y1, r, 8)
    c_zl = c + 1 - 2 * zl
    c_x1, c_x3, _ = near(x0, x1, c, 2)
    zi1, zi3, zi2 = near(z0, z1, zh, 1)
    yi1, yi3, yi2 = near(y0, y1, y, 1)
    xi1, xi3, xi2 = near(x0, x1, x, 1)
    zlo = 1 - zl
    coreo = 1 - core
    dev = {"core": (r_core, c), "z1": (r_z1, c), "z3": (r_z3, c), "y1": (r_y1, c), "y3": (r_y3, c),
           "zl": (r, c_zl), "x1": (r, c_x1), "x3": (r, c_x3)}

    nsem = [0]
    sends = []

    def rc(src, dst, peer, rs=None, keep=True):
        i = nsem[0]
        nsem[0] += 1
        d = pltpu.make_async_remote_copy(src_ref=src, dst_ref=dst, send_sem=ssem.at[i],
                                         recv_sem=rsem.at[i if rs is None else rs],
                                         device_id=dev[peer], device_id_type=MESH)
        if keep:
            sends.append(d)
        return d

    def go(*a):
        d = rc(*a)
        d.start()
        return d

    bar = pltpu.get_barrier_semaphore()
    for p in dev.values():
        pl.semaphore_signal(bar, inc=1, device_id=p, device_id_type=MESH)
    pl.semaphore_wait(bar, len(dev))

    class Gather4:
        def __init__(self, own, slot, me, i1, i3, p1, p3):
            self.slot, self.i, self.p = slot, (me, i1, i3), (p1, p3)
            self.c1 = go(own(0), slot(me, 0), p1)
            self.c2 = go(own(1), slot(me, 1), p3)
            self.c3 = go(own(1), slot(me, 1), p1)
            self.c4 = go(own(0), slot(me, 0), p3)

        def forward(self):
            (_, i1, i3), (p1, p3) = self.i, self.p
            self.c1.wait_recv()
            self.f1 = go(self.slot(i1, 0), self.slot(i1, 0), p3)
            self.c2.wait_recv()
            self.f2 = go(self.slot(i3, 1), self.slot(i3, 1), p1)

        def near(self):
            self.c3.wait_recv()
            self.c4.wait_recv()

        def far(self):
            self.f1.wait_recv()
            self.f2.wait_recv()

    d_zl = go(di, DS.at[y, x, zl], "zl")
    wbs = []
    for q in range(4):
        cols = pl.ds(q * 128, 128)
        wbs.append((go(wb.at[:, cols], WB.at[1, q, 0:KD], "zl"),
                    go(g.at[:, cols], WB.at[1, q, KD:KP], "zl")))
    loc = []

    def lc(src, dst):
        d = pltpu.make_async_copy(src, dst, lsem.at[len(loc)])
        d.start()
        loc.append(d)

    lc(di, DS.at[y, x, zl])
    for q in range(4):
        cols = pl.ds(q * 128, 128)
        lc(wb.at[:, cols], WB.at[0, q, 0:KD])
        lc(g.at[:, cols], WB.at[0, q, KD:KP])
    lc(ft, FT.at[x])
    for d in loc:
        d.wait()

    d_zl.wait_recv()
    half_k = KD // 2
    dx = Gather4(lambda h: DS.at[y, x, h], lambda i, h: DS.at[y, i, h], x, xi1, xi3, "x1", "x3")
    dx.forward()
    dx.near()
    fx = Gather4(lambda h: FT.at[x, h * half_k:(h + 1) * half_k],
                 lambda i, h: FT.at[i, h * half_k:(h + 1) * half_k], x, xi1, xi3, "x1", "x3")
    dx.far()
    dy = Gather4(lambda h: DS.at[y, 2 * h:2 * h + 2], lambda i, h: DS.at[i, 2 * h:2 * h + 2],
                 y, yi1, yi3, "y1", "y3")

    def gray(i):
        return (i % 2 + i // 2) % 2, i // 2

    def transpose_in(h, q):
        g1, g2 = gray(q)
        pos = (2 * g1 + g2, 2 * g2 + g1)

        def step(i, _):
            k = pl.multiple_of(i * 256, 256)
            hi, lo = split(WB[h, q, pl.ds(k, 256), :].T)
            for ck in range(2):
                for ab in range(2):
                    s = ck * 64 + ab * 32
                    t = ab * 128 + pos[ab] * 32
                    WTh[ck, t:t + 32, pl.ds(k, 256)] = hi[s:s + 32]
                    WTl[ck, t:t + 32, pl.ds(k, 256)] = lo[s:s + 32]
            return 0

        lax.fori_loop(0, KP // 256, step, 0)

    def convert(i):
        def step(j, _):
            k = pl.multiple_of(j * 64, 64)
            hi, lo = split(FT[i, pl.ds(k, 64), :])
            FTh[i, pl.ds(k, 64), :] = hi
            FTl[i, pl.ds(k, 64), :] = lo
            return 0

        lax.fori_loop(0, KD // 64, step, 0)
        a = lax.broadcasted_iota(jnp.int32, (64, 256), 0)
        b = lax.broadcasted_iota(jnp.int32, (64, 256), 1)
        mine = jnp.where(jnp.logical_and(i == y, zl == z1), 1, 0)
        e = jnp.where(b == a + (2 * z0 + core) * 64, mine, 0).astype(F32)
        FTh[i, KD:KP, :] = (-e).astype(BF16)
        FTl[i, KD:KP, :] = jnp.zeros((64, 256), BF16)

    def product(h, i, m):
        cols = pl.ds(pl.multiple_of(m * 256, 256), 256)

        def step(ck, _):
            PT[h, ck, :, cols] = mm3(WTh[ck], WTl[ck], FTh[i], FTl[i], ((1,), (0,)))
            return 0

        lax.fori_loop(0, 2, step, 0)

    for q in range(4):
        transpose_in(0, q)
    convert(x)
    product(0, x, x)
    dy.forward()
    fx.forward()
    fx.near()
    for i in (xi1, xi3):
        convert(i)
        product(0, i, i)
    fx.far()
    convert(xi2)
    product(0, xi2, xi2)
    dy.near()
    dy.far()

    u1, u2 = (y0 + y1) % 2, y1
    v1, v2 = (z0 + z1) % 2, z1

    def al(v, n):
        return pl.multiple_of(v, n)

    def reduce_to_owner(h):
        own = PT.at[h, core]
        d = go(PT.at[h, coreo], RC.at[h], "core")
        d.wait_recv()

        def add_core(i, _):
            s = pl.ds(al(i * 32, 32), 32)
            PT[h, core, s, :] = PT[h, core, s, :] + RC[h, s, :]
            return 0

        lax.fori_loop(0, 8, add_core, 0)

        def exchange(offs, size, buf, first, second, keeps):
            ds_ = []
            for ab in range(2):
                src = own.at[pl.ds(al(offs[ab] + (1 - keeps[ab]) * size, size), size)]
                ds_.append(go(src, buf.at[h, ab], (first, second)[ab]))
            new = [al(offs[ab] + keeps[ab] * size, size) for ab in range(2)]
            for ab in range(2):
                ds_[ab].wait_recv()
                s = pl.ds(new[ab], size)
                PT[h, core, s, :] = PT[h, core, s, :] + buf[h, ab]
            return new

        offs = exchange([0, 128], 64, RY1, "y1", "y3", (u1, u2))
        offs = exchange(offs, 32, RY2, "y3", "y1", (u2, u1))
        offs = exchange(offs, 16, RZ1, "z1", "z3", (v1, v2))
        return exchange(offs, 8, RZ2, "z3", "z1", (v2, v1))

    offs0 = reduce_to_owner(0)
    for q in range(4):
        for d in wbs[q]:
            d.wait_recv()
        transpose_in(1, q)

    def product_all(i, _):
        product(1, i, i)
        return 0

    lax.fori_loop(0, 4, product_all, 0)

    def dsplit(q, _):
        for j in range(8):
            hi, lo = split(DS[q, j // 2, j % 2])
            lanes = pl.ds((j % 2) * 1024 + (j // 2) * 256, 256)
            DSh[0, pl.ds(al(q * 64, 64), 64), lanes] = hi
            DSh[1, pl.ds(al(q * 64, 64), 64), lanes] = lo
        return 0

    offs1 = reduce_to_owner(1)

    rows_a = core * 64 + v1 * 16 + v2 * 8
    rows_b = core * 64 + 32 + v2 * 16 + v1 * 8
    rows = [al(rows_a, 8), al(rows_b, 8)]
    xz = []
    for ab in range(2):
        xz.append(go(PT.at[1, core, pl.ds(offs1[ab], 8)], RG.at[zl, pl.ds(rows[ab], 8)], "zl"))
        RG[zl, pl.ds(rows[ab], 8), :] = PT[0, core, pl.ds(offs0[ab], 8), :]
    lax.fori_loop(0, 4, dsplit, 0)
    for d in xz:
        d.wait_recv()

    def widen(starts, size, peers):
        ds_ = []
        for ab in range(2):
            s = pl.ds(al(starts[ab], size), size)
            ds_.append(go(RG.at[:, s], RG.at[:, s], peers[ab]))
        for d in ds_:
            d.wait_recv()

    widen(rows, 8, ("z3", "z1"))
    widen([core * 64 + v1 * 16, core * 64 + 32 + v2 * 16], 16, ("z1", "z3"))
    s = pl.ds(al(core * 64, 64), 64)
    go(RG.at[:, s], RG.at[:, s], "core").wait_recv()

    acc = None
    for j in range(2):
        rh, rl = split(RG[j])
        lanes = pl.ds(j * 1024, 1024)
        t = mm3(DSh[0, :, lanes], DSh[1, :, lanes], rh, rl, ((1,), (1,)))
        acc = t if acc is None else acc + t
    WA[core, y, zh] = -acc

    wz = Gather4(lambda h: WA.at[core, y, zh, 128 * h:128 * h + 128],
                 lambda i, h: WA.at[core, y, i, 128 * h:128 * h + 128], zh, zi1, zi3, "z1", "z3")
    wz.forward()
    wz.near()
    wz.far()
    wy = Gather4(lambda h: WA.at[core, y, 2 * h:2 * h + 2], lambda i, h: WA.at[core, i, 2 * h:2 * h + 2],
                 y, yi1, yi3, "y1", "y3")
    wc = [go(WA.at[core, y], WA.at[core, y], "core")]
    wy.forward()
    wy.near()
    for i in (yi1, yi3):
        wc.append(go(WA.at[core, i], WA.at[core, i], "core"))
    wy.far()
    wc.append(go(WA.at[core, yi2], WA.at[core, yi2], "core"))

    for q in range(4):
        w_out[:, q * 128:(q + 1) * 128] = WA[core, q, zh, pl.ds(al(y * 64, 64), 64), :]
    for d in wc:
        d.wait_recv()

    y2 = 2 * z0 + core
    d1 = (x0 + x1 + y0 + y1) % 2
    d2 = (x1 + y1) % 2
    dz = (zl + z1) % 2
    base = nsem[0]
    cp = {}
    for p in ("x1", "x3", "zl"):
        for t in range(4):
            piece = LB.at[t // 2, 2 * (t % 2):2 * (t % 2) + 2]
            src = WA.at[t // 2, y2, 2 * (t % 2):2 * (t % 2) + 2]
            i = nsem[0]
            nsem[0] += 1
            for from_wa in (True, False):
                cp[p, t, from_wa] = pltpu.make_async_remote_copy(
                    src_ref=src if from_wa else piece, dst_ref=piece, send_sem=ssem.at[i],
                    recv_sem=rsem.at[base + t], device_id=dev[p], device_id_type=MESH)

    code = dz * 4 + d2 * 2 + d1

    @pl.when(code == 0)
    def _():
        for a, b, zz in ((0, 2, 0), (1, 3, 2), (2, 0, 1), (3, 1, 3)):
            cp["x1", a, True].start()
            cp["x3", b, True].start()
            cp["zl", zz, True].start()
        for t in range(2):
            for q in range(4):
                LB[t, q] = WA[t, y2, q]
        for p in ("x1", "x3", "zl"):
            for t in range(4):
                cp[p, t, True].wait_send()

    def relay(order, onward):
        for t in order:
            cp["zl", t, False].wait_recv()
            if t in onward:
                cp[onward[t], t, False].start()
            cp["zl", t, False].start()
        for t in order:
            if t in onward:
                cp[onward[t], t, False].wait_send()
            cp["zl", t, False].wait_send()

    @pl.when(code == 1)
    def _():
        relay((0, 1, 2, 3), {0: "x3", 1: "x3"})

    @pl.when(code == 2)
    def _():
        relay((2, 3, 0, 1), {2: "x1", 3: "x1"})

    @pl.when(code == 3)
    def _():
        relay((0, 2, 1, 3), {})

    @pl.when(dz == 1)
    def _():
        for t in range(4):
            cp["zl", t, False].wait_recv()

    gram_out[...] = jnp.zeros_like(gram_out)

    def gram_step(i, _):
        a, b = i // 4, i % 4
        lh, ll = split(LB[a, b].T)
        for q in range(4):
            rh, rl = split(WA[a, q, b])
            lanes = slice(q * 128, (q + 1) * 128)
            gram_out[:, lanes] = gram_out[:, lanes] + mm3(lh, ll, rh, rl, ((1,), (0,)))
        return 0

    lax.fori_loop(0, 8, gram_step, 0)
    gram_out[...] = gram_out[...] * (1.0 / ROWS)
    for d in sends:
        d.wait_send()
    assert nsem[0] <= NSEM


def body(f, wb, g, di):
    ft = f.T
    vm, dma = pltpu.VMEM, pltpu.SemaphoreType.DMA
    return pl.pallas_call(
        kernel,
        out_shape=(jax.ShapeDtypeStruct((64, 512), F32), jax.ShapeDtypeStruct((128, 512), F32)),
        in_specs=[pl.BlockSpec(memory_space=pl.ANY)] * 4,
        out_specs=(pl.BlockSpec(memory_space=pltpu.VMEM),) * 2,
        scratch_shapes=[
            vm((4, KD, 256), F32), vm((4, KP, 256), BF16), vm((4, KP, 256), BF16),
            vm((2, 4, KP, 128), F32), vm((2, 256, KP), BF16), vm((2, 256, KP), BF16),
            vm((2, 2, 256, 1024), F32), vm((2, 256, 1024), F32),
            vm((2, 2, 64, 1024), F32), vm((2, 2, 32, 1024), F32),
            vm((2, 2, 16, 1024), F32), vm((2, 2, 8, 1024), F32),
            vm((2, 128, 1024), F32), vm((4, 4, 2, 64, 256), F32), vm((2, 256, 2048), BF16),
            vm((2, 4, 4, 256, 128), F32), vm((2, 4, 256, 128), F32),
            dma((NSEM,)), dma((NSEM,)), dma((10,)),
        ],
        compiler_params=pltpu.CompilerParams(collective_id=0, has_side_effects=True,
                                             vmem_limit_bytes=66_000_000),
        name="panel",
    )(ft, wb, g, di)


def solution(mesh):
    return jax.shard_map(
        body, mesh=mesh,
        in_specs=(P("pcol", "prow"), P("prow", "pcol"), P("prow", "pcol"), P("prow", "pcol")),
        out_specs=(P("prow", "pcol"), P("prow", "pcol")), check_vma=False)
```

```python
import jax
import jax.numpy as jnp
from jax import lax
from jax.experimental import pallas as pl
from jax.experimental.pallas import tpu as pltpu
from jax.sharding import PartitionSpec as P

F32 = jnp.float32
BF16 = jnp.bfloat16
MESH = pl.DeviceIdType.MESH
ROWS = 2048
KD = 1984
KP = 2048
NSEM = 140
CUTS = (0, 512, 1024, 1536, 1792, KD)


def split(v):
    hi = v.astype(BF16)
    return hi, (v - hi.astype(F32)).astype(BF16)


def mm(a, b, dims):
    return lax.dot_general(a, b, (dims, ((), ())), preferred_element_type=F32)


def mm3(ah, al, bh, bl, dims):
    return mm(ah, bh, dims) + (mm(ah, bl, dims) + mm(al, bh, dims))


def kernel(ft, wb, g, di, w_out, gram_out, FT, FTh, FTl, WB, WTh, WTl, PT, RC, RYa, RYb,
           RZa, RZb, RG, DS, DSh, WA, LB, TW, ssem, rsem, lsem):
    r = lax.axis_index("prow")
    c = lax.axis_index("pcol")
    core = r % 2
    z0, z1 = (r // 2) % 2, (r // 4) % 2
    y0, y1 = (r // 8) % 2, r // 16
    zl = c % 2
    x0, x1 = (c // 2) % 2, c // 4
    zh, y, x = z0 + 2 * z1, y0 + 2 * y1, x0 + 2 * x1

    def near(b0, b1, base, unit):
        p1 = base + unit * (1 - 2 * b0)
        return p1, p1 + 2 * unit * (1 - 2 * b1), base + 2 * unit * (1 - 2 * b1)

    r_core = r + 1 - 2 * core
    r_z1, r_z3, _ = near(z0, z1, r, 2)
    r_y1, r_y3, _ = near(y0, y1, r, 8)
    c_zl = c + 1 - 2 * zl
    c_x1, c_x3, _ = near(x0, x1, c, 2)
    zi1, zi3, zi2 = near(z0, z1, zh, 1)
    yi1, yi3, yi2 = near(y0, y1, y, 1)
    xi1, xi3, xi2 = near(x0, x1, x, 1)
    zlo = 1 - zl
    coreo = 1 - core
    dev = {"core": (r_core, c), "z1": (r_z1, c), "z3": (r_z3, c), "y1": (r_y1, c), "y3": (r_y3, c),
           "zl": (r, c_zl), "x1": (r, c_x1), "x3": (r, c_x3)}

    nsem = [0]
    sends = []

    def rc(src, dst, peer, rs=None, keep=True):
        i = nsem[0]
        nsem[0] += 1
        d = pltpu.make_async_remote_copy(src_ref=src, dst_ref=dst, send_sem=ssem.at[i],
                                         recv_sem=rsem.at[i if rs is None else rs],
                                         device_id=dev[peer], device_id_type=MESH)
        if keep:
            sends.append(d)
        return d

    def go(*a):
        d = rc(*a)
        d.start()
        return d

    bar = pltpu.get_barrier_semaphore()
    for p in dev.values():
        pl.semaphore_signal(bar, inc=1, device_id=p, device_id_type=MESH)
    pl.semaphore_wait(bar, len(dev))

    class Gather4:
        def __init__(self, own, slot, me, i1, i3, p1, p3):
            self.slot, self.i, self.p = slot, (me, i1, i3), (p1, p3)
            self.c1 = go(own(0), slot(me, 0), p1)
            self.c2 = go(own(1), slot(me, 1), p3)
            self.c3 = go(own(1), slot(me, 1), p1)
            self.c4 = go(own(0), slot(me, 0), p3)

        def forward(self):
            (_, i1, i3), (p1, p3) = self.i, self.p
            self.c1.wait_recv()
            self.f1 = go(self.slot(i1, 0), self.slot(i1, 0), p3)
            self.c2.wait_recv()
            self.f2 = go(self.slot(i3, 1), self.slot(i3, 1), p1)

        def near(self):
            self.c3.wait_recv()
            self.c4.wait_recv()

        def far(self):
            self.f1.wait_recv()
            self.f2.wait_recv()

    d_zl = go(di, DS.at[y, x, zl], "zl")
    d_g = go(g, WB.at[1, KD:KP], "zl")
    wbs = [go(wb.at[a:b], WB.at[1, a:b], "zl") for a, b in zip(CUTS[:-1], CUTS[1:])]
    loc = []

    def lc(src, dst):
        d = pltpu.make_async_copy(src, dst, lsem.at[len(loc)])
        d.start()
        loc.append(d)

    lc(di, DS.at[y, x, zl])
    lc(wb, WB.at[0, 0:KD])
    lc(g, WB.at[0, KD:KP])
    lc(ft, FT.at[x])
    for d in loc:
        d.wait()

    d_zl.wait_recv()
    half_k = KD // 2
    dx = Gather4(lambda h: DS.at[y, x, h], lambda i, h: DS.at[y, i, h], x, xi1, xi3, "x1", "x3")
    dx.forward()
    dx.near()
    fx = Gather4(lambda h: FT.at[x, h * half_k:(h + 1) * half_k],
                 lambda i, h: FT.at[i, h * half_k:(h + 1) * half_k], x, xi1, xi3, "x1", "x3")
    dx.far()
    dy = Gather4(lambda h: DS.at[y, 2 * h:2 * h + 2], lambda i, h: DS.at[i, 2 * h:2 * h + 2],
                 y, yi1, yi3, "y1", "y3")

    def transpose_in(h, q, k0, k1):
        qi = 2 * ((q % 2 + q // 2) % 2) + q // 2

        def step(i, _):
            k = pl.multiple_of(i * 256, 256)
            hi, lo = split(WB[h, pl.ds(k, 256), q * 128:(q + 1) * 128].T)
            for s in range(2):
                for ck in range(2):
                    f = s * 64 + ck * 32
                    t = ck * 128 + qi * 32
                    WTh[s, t:t + 32, pl.ds(k, 256)] = hi[f:f + 32]
                    WTl[s, t:t + 32, pl.ds(k, 256)] = lo[f:f + 32]
            return 0

        lax.fori_loop(k0 // 256, k1 // 256, step, 0)

    def convert(i):
        def step(j, _):
            k = pl.multiple_of(j * 64, 64)
            hi, lo = split(FT[i, pl.ds(k, 64), :])
            FTh[i, pl.ds(k, 64), :] = hi
            FTl[i, pl.ds(k, 64), :] = lo
            return 0

        lax.fori_loop(0, KD // 64, step, 0)
        a = lax.broadcasted_iota(jnp.int32, (64, 256), 0)
        b = lax.broadcasted_iota(jnp.int32, (64, 256), 1)
        mine = jnp.where(jnp.logical_and(i == y, zl == z1), 1, 0)
        e = jnp.where(b == a + (2 * z0 + core) * 64, mine, 0).astype(F32)
        FTh[i, KD:KP, :] = (-e).astype(BF16)
        FTl[i, KD:KP, :] = jnp.zeros((64, 256), BF16)

    def product(h, i, m, k0, k1, s_all, add):
        cols = pl.ds(pl.multiple_of(m * 256, 256), 256)

        def step(s, _):
            t = mm3(WTh[s, :, k0:k1], WTl[s, :, k0:k1], FTh[i, k0:k1], FTl[i, k0:k1], ((1,), (0,)))
            t = t.reshape(2, 2, 2, 2, 2, 8, 256)
            at = (s, h) + (slice(None),) * 6 + (cols,)
            PT[at] = PT[at] + t if add else t
            return 0

        lax.fori_loop(s_all[0], s_all[-1] + 1, step, 0)

    def product_all(h, k0, k1, s_all, add):
        def one(i, _):
            product(h, i, i, k0, k1, s_all, add)
            return 0

        lax.fori_loop(0, 4, one, 0)

    both = (0, 1)
    for q in range(4):
        transpose_in(0, q, 0, KP)
    convert(x)
    product(0, x, x, 0, KP, both, False)
    dy.forward()
    fx.forward()
    fx.near()
    for i in (xi1, xi3):
        convert(i)
        product(0, i, i, 0, KP, both, False)
    fx.far()
    convert(xi2)
    product(0, xi2, xi2, 0, KP, both, False)

    u1, u2 = (y0 + y1) % 2, y1
    v1, v2 = (z0 + z1) % 2, z1

    def al(v, n):
        return pl.multiple_of(v, n)

    LA, LB_ = slice(0, 512), slice(512, 1024)
    every = slice(None)

    def reduce_to_owner(s, h):
        d = go(PT.at[s, h, coreo], RC.at[s, h], "core")
        yield
        d.wait_recv()
        for i in range(2):
            PT[s, h, core, i] = PT[s, h, core, i] + RC[s, h, i]

        def swap(buf, a_to, a_send, a_keep, b_to, b_send, b_keep):
            def part(i, lanes):
                return (s, h, core) + i + (every,) * (5 - len(i)) + (lanes,)

            da = go(PT.at[part(a_send, LA)], buf.at[s, h, 0], a_to)
            db = go(PT.at[part(b_send, LB_)], buf.at[s, h, 1], b_to)
            yield
            for d_, keep, lanes, i in ((da, a_keep, LA, 0), (db, b_keep, LB_, 1)):
                d_.wait_recv()
                at = part(keep, lanes)
                PT[at] = PT[at] + buf[s, h, i]

        def full(*idx):
            return idx

        yield from swap(RYa, "y1", full(1 - u1), full(u1), "y3", full(every, 1 - u2), full(every, u2))
        yield from swap(RYb, "y3", full(u1, 1 - u2), full(u1, u2), "y1", full(1 - u1, u2), full(u1, u2))
        yield from swap(RZa, "z1", full(u1, u2, 1 - v1), full(u1, u2, v1),
                        "z3", full(u1, u2, every, 1 - v2), full(u1, u2, every, v2))
        yield from swap(RZb, "z3", full(u1, u2, v1, 1 - v2), full(u1, u2, v1, v2),
                        "z1", full(u1, u2, 1 - v1, v2), full(u1, u2, v1, v2))

    code = ((zl + z1) % 2) * 4 + ((x1 + y1) % 2) * 2 + (x0 + x1 + y0 + y1) % 2
    y2 = 2 * z0 + core
    last = []

    def spread(s):
        base = nsem[0]
        nsem[0] += 12

        def cp(p, t, from_wa):
            at = pl.ds(2 * (t % 2), 2)
            piece = LB.at[s, t // 2, at]
            return pltpu.make_async_remote_copy(
                src_ref=WA.at[s, t // 2, y2, at] if from_wa else piece, dst_ref=piece,
                send_sem=ssem.at[base + 4 * ("x1", "x3", "zl").index(p) + t],
                recv_sem=rsem.at[base + t], device_id=dev[p], device_id_type=MESH)

        @pl.when(code == 0)
        def _():
            for a, b, zz in ((0, 2, 0), (1, 3, 2), (2, 0, 1), (3, 1, 3)):
                cp("x1", a, True).start()
                cp("x3", b, True).start()
                cp("zl", zz, True).start()
            for t in range(2):
                for q in range(4):
                    LB[s, t, q] = WA[s, t, y2, q]

        roles = {1: ((0, 1, 2, 3), {0: "x3", 1: "x3"}), 2: ((2, 3, 0, 1), {2: "x1", 3: "x1"}),
                 3: ((0, 2, 1, 3), {})}
        for n in range(4):
            yield
            for k, (order, onward) in roles.items():
                @pl.when(code == k)
                def _(order=order, onward=onward):
                    t = order[n]
                    cp("zl", t, False).wait_recv()
                    if t in onward:
                        cp(onward[t], t, False).start()
                    cp("zl", t, False).start()

            @pl.when(code >= 4)
            def _():
                cp("zl", (0, 2, 1, 3)[n], False).wait_recv()

        def finish():
            @pl.when(code == 0)
            def _():
                for p in ("x1", "x3", "zl"):
                    for t in range(4):
                        cp(p, t, True).wait_send()

            for k, (order, onward) in roles.items():
                @pl.when(code == k)
                def _(onward=onward):
                    for t in range(4):
                        if t in onward:
                            cp(onward[t], t, False).wait_send()
                        cp("zl", t, False).wait_send()

        last.append(finish)

    def stream(s):
        yield from reduce_to_owner(s, 1)
        d = go(PT.at[s, 1, core, u1, u2, v1, v2], RG.at[s, zl, core, v1, v2], "zl")
        RG[s, zl, core, v1, v2] = PT[s, 0, core, u1, u2, v1, v2]
        yield
        d.wait_recv()

        def widen(*moves):
            ds_ = [go(RG.at[(s, every, core) + i + (every, lanes)],
                      RG.at[(s, every, core) + i + (every, lanes)], p) for i, lanes, p in moves]
            yield
            for d_ in ds_:
                d_.wait_recv()

        yield from widen(((v1, v2), LA, "z3"), ((v1, v2), LB_, "z1"))
        yield from widen(((v1, every), LA, "z1"), ((every, v2), LB_, "z3"))
        d = go(RG.at[s, :, core], RG.at[s, :, core], "core")
        yield
        d.wait_recv()
        acc = None
        for j in range(2):
            rh, rl = split(RG[s, j].reshape(64, 1024))
            lanes = pl.ds(j * 1024, 1024)
            t = mm3(rh, rl, DSh[0, :, lanes], DSh[1, :, lanes], ((1,), (1,)))
            acc = t if acc is None else acc + t
        WA[s, core, y, zh] = -acc

        wz = Gather4(lambda h: WA.at[s, core, y, zh, 32 * h:32 * h + 32],
                     lambda i, h: WA.at[s, core, y, i, 32 * h:32 * h + 32], zh, zi1, zi3, "z1", "z3")
        yield
        wz.forward()
        yield
        wz.near()
        wz.far()
        wy = Gather4(lambda h: WA.at[s, core, y, 2 * h:2 * h + 2],
                     lambda i, h: WA.at[s, core, i, 2 * h:2 * h + 2], y, yi1, yi3, "y1", "y3")
        wc = [go(WA.at[s, core, y], WA.at[s, core, y], "core")]
        yield
        wy.forward()
        yield
        wy.near()
        for i in (yi1, yi3):
            wc.append(go(WA.at[s, core, i], WA.at[s, core, i], "core"))
        yield
        wy.far()
        wc.append(go(WA.at[s, core, yi2], WA.at[s, core, yi2], "core"))
        yield
        for d in wc:
            d.wait_recv()
        yield from spread(s)

    def advance(*gens):
        for i in gens:
            next(i)

    early = [reduce_to_owner(0, 0), reduce_to_owner(1, 0)]
    advance(*early)
    d_g.wait_recv()
    for i in range(3):
        wbs[i].wait_recv()
    for q in range(4):
        transpose_in(1, q, 0, 1536)
    advance(*early)
    product_all(1, 0, 1536, both, False)
    advance(*early)

    def dsplit(q, _):
        for j in range(8):
            hi, lo = split(DS[q, j // 2, j % 2])
            lanes = pl.ds((j % 2) * 1024 + (j // 2) * 256, 256)
            DSh[0, pl.ds(al(q * 64, 64), 64), lanes] = hi
            DSh[1, pl.ds(al(q * 64, 64), 64), lanes] = lo
        return 0

    dy.near()
    dy.far()
    lax.fori_loop(0, 4, dsplit, 0)
    wbs[3].wait_recv()
    for q in range(4):
        transpose_in(1, q, 1536, 1792)
    product_all(1, 1536, 1792, both, True)
    advance(*early)
    wbs[4].wait_recv()
    for q in range(4):
        transpose_in(1, q, 1792, KP)
    streams = [stream(0), stream(1)]
    for s in range(2):
        product_all(1, 1792, KP, (s,), True)
        advance(streams[s])
    pending = early + streams
    while pending:
        for i in list(pending):
            if next(i, "end") == "end":
                pending.remove(i)

    for q in range(4):
        blk = pl.ds(al(y1 * 128, 128), 128)
        TW[q] = jnp.concatenate([WA[0, core, q, zh, :, blk], WA[1, core, q, zh, :, blk]], axis=0).T
        w_out[:, q * 128:(q + 1) * 128] = TW[q, pl.ds(al(y0 * 64, 64), 64), :]

    gram_out[...] = jnp.zeros_like(gram_out)

    def gram_step(i, _):
        a, b = i // 4, i % 4
        lh, ll = split(jnp.concatenate([LB[0, a, b], LB[1, a, b]], axis=0))
        rh, rl = split(jnp.concatenate([WA[s, a, q, b] for q in range(4) for s in range(2)], axis=0))
        gram_out[...] = gram_out[...] + mm3(lh, ll, rh, rl, ((1,), (1,)))
        return 0

    lax.fori_loop(0, 8, gram_step, 0)
    gram_out[...] = gram_out[...] * (1.0 / ROWS)
    for d in sends:
        d.wait_send()
    for end in last:
        end()
    assert nsem[0] <= NSEM


def body(f, wb, g, di):
    ft = f.T
    vm, dma = pltpu.VMEM, pltpu.SemaphoreType.DMA
    return pl.pallas_call(
        kernel,
        out_shape=(jax.ShapeDtypeStruct((64, 512), F32), jax.ShapeDtypeStruct((128, 512), F32)),
        in_specs=[pl.BlockSpec(memory_space=pl.ANY)] * 4,
        out_specs=(pl.BlockSpec(memory_space=pltpu.VMEM),) * 2,
        scratch_shapes=[
            vm((4, KD, 256), F32), vm((4, KP, 256), BF16), vm((4, KP, 256), BF16),
            vm((2, KP, 512), F32), vm((2, 256, KP), BF16), vm((2, 256, KP), BF16),
            vm((2, 2, 2, 2, 2, 2, 2, 8, 1024), F32), vm((2, 2, 2, 2, 2, 2, 8, 1024), F32),
            vm((2, 2, 2, 2, 2, 2, 8, 512), F32), vm((2, 2, 2, 2, 2, 8, 512), F32),
            vm((2, 2, 2, 2, 8, 512), F32), vm((2, 2, 2, 8, 512), F32),
            vm((2, 2, 2, 2, 2, 8, 1024), F32), vm((4, 4, 2, 64, 256), F32), vm((2, 256, 2048), BF16),
            vm((2, 2, 4, 4, 64, 256), F32), vm((2, 2, 4, 64, 256), F32), vm((4, 128, 128), F32),
            dma((NSEM,)), dma((NSEM,)), dma((10,)),
        ],
        compiler_params=pltpu.CompilerParams(collective_id=0, has_side_effects=True,
                                             vmem_limit_bytes=66_000_000),
        name="panel",
    )(ft, wb, g, di)


def solution(mesh):
    return jax.shard_map(
        body, mesh=mesh,
        in_specs=(P("pcol", "prow"), P("prow", "pcol"), P("prow", "pcol"), P("prow", "pcol")),
        out_specs=(P("prow", "pcol"), P("prow", "pcol")), check_vma=False)
```

```python
import jax
import jax.numpy as jnp
from jax import lax
from jax.experimental import pallas as pl
from jax.experimental.pallas import tpu as pltpu
from jax.sharding import PartitionSpec as P

F32 = jnp.float32
BF16 = jnp.bfloat16
MESH = pl.DeviceIdType.MESH
ROWS = 2048
KD = 1984
KP = 2048
NSEM = 140
CUTS = (0, 512, 1024, 1536, KD)


def split(v):
    hi = v.astype(BF16)
    return hi, (v - hi.astype(F32)).astype(BF16)


def mm(a, b, dims):
    return lax.dot_general(a, b, (dims, ((), ())), preferred_element_type=F32)


def mm3(ah, al, bh, bl, dims):
    return mm(ah, bh, dims) + (mm(ah, bl, dims) + mm(al, bh, dims))


def kernel(ft, wb, g, di, w_out, gram_out, FT, FTh, FTl, WB, OT, IT, WTh, WTl, PT, RC, RYa, RYb,
           RZa, RZb, RG, DS, DSh, WA, LB, TW, ssem, rsem, lsem):
    r = lax.axis_index("prow")
    c = lax.axis_index("pcol")
    core = r % 2
    z0, z1 = (r // 2) % 2, (r // 4) % 2
    y0, y1 = (r // 8) % 2, r // 16
    zl = c % 2
    x0, x1 = (c // 2) % 2, c // 4
    zh, y, x = z0 + 2 * z1, y0 + 2 * y1, x0 + 2 * x1

    def near(b0, b1, base, unit):
        p1 = base + unit * (1 - 2 * b0)
        return p1, p1 + 2 * unit * (1 - 2 * b1), base + 2 * unit * (1 - 2 * b1)

    r_core = r + 1 - 2 * core
    r_z1, r_z3, _ = near(z0, z1, r, 2)
    r_y1, r_y3, _ = near(y0, y1, r, 8)
    c_zl = c + 1 - 2 * zl
    c_x1, c_x3, _ = near(x0, x1, c, 2)
    zi1, zi3, zi2 = near(z0, z1, zh, 1)
    yi1, yi3, yi2 = near(y0, y1, y, 1)
    xi1, xi3, xi2 = near(x0, x1, x, 1)
    zlo = 1 - zl
    coreo = 1 - core
    dev = {"core": (r_core, c), "z1": (r_z1, c), "z3": (r_z3, c), "y1": (r_y1, c), "y3": (r_y3, c),
           "zl": (r, c_zl), "x1": (r, c_x1), "x3": (r, c_x3)}

    nsem = [0]
    sends = []

    def rc(src, dst, peer, rs=None, keep=True):
        i = nsem[0]
        nsem[0] += 1
        d = pltpu.make_async_remote_copy(src_ref=src, dst_ref=dst, send_sem=ssem.at[i],
                                         recv_sem=rsem.at[i if rs is None else rs],
                                         device_id=dev[peer], device_id_type=MESH)
        if keep:
            sends.append(d)
        return d

    def go(*a):
        d = rc(*a)
        d.start()
        return d

    bar = pltpu.get_barrier_semaphore()
    for p in dev.values():
        pl.semaphore_signal(bar, inc=1, device_id=p, device_id_type=MESH)
    pl.semaphore_wait(bar, len(dev))

    class Gather4:
        def __init__(self, own, slot, me, i1, i3, p1, p3):
            self.slot, self.i, self.p = slot, (me, i1, i3), (p1, p3)
            self.c1 = go(own(0), slot(me, 0), p1)
            self.c2 = go(own(1), slot(me, 1), p3)
            self.c3 = go(own(1), slot(me, 1), p1)
            self.c4 = go(own(0), slot(me, 0), p3)

        def forward(self):
            (_, i1, i3), (p1, p3) = self.i, self.p
            self.c1.wait_recv()
            self.f1 = go(self.slot(i1, 0), self.slot(i1, 0), p3)
            self.c2.wait_recv()
            self.f2 = go(self.slot(i3, 1), self.slot(i3, 1), p1)

        def near(self):
            self.c3.wait_recv()
            self.c4.wait_recv()

        def far(self):
            self.f1.wait_recv()
            self.f2.wait_recv()

    d_zl = go(di, DS.at[y, x, zl], "zl")
    loc = []

    def lc(src, dst):
        d = pltpu.make_async_copy(src, dst, lsem.at[len(loc)])
        d.start()
        loc.append(d)

    for a, b in zip(CUTS[:-1], CUTS[1:]):
        lc(wb.at[a:b], WB.at[a:b])
    lc(g, WB.at[KD:KP])
    lc(di, DS.at[y, x, zl])
    lc(ft, FT.at[x])

    def transpose_in(k0, k1):
        def step(i, _):
            k = pl.multiple_of(i * 256, 256)
            at = pl.ds(k, 256)
            for q in range(4):
                qi = 2 * ((q % 2 + q // 2) % 2) + q // 2
                v = WB[at, q * 128:(q + 1) * 128].T
                hi, lo = split(v)
                for s in range(2):
                    for ck in range(2):
                        f = slice(s * 64 + ck * 32, s * 64 + ck * 32 + 32)
                        t = slice(ck * 128 + qi * 32, ck * 128 + qi * 32 + 32)
                        OT[s, t, at] = v[f]
                        WTh[0, s, t, at] = hi[f]
                        WTl[0, s, t, at] = lo[f]
            return 0

        lax.fori_loop(k0 // 256, k1 // 256, step, 0)

    def swap_w(s, k0, k1):
        return go(OT.at[s, :, k0:k1], IT.at[s, :, k0:k1], "zl")

    def split_in(s, k0, k1):
        def step(i, _):
            at = pl.ds(pl.multiple_of(i * 32, 32), 32)
            hi, lo = split(IT[s, at, k0:k1])
            WTh[1, s, at, k0:k1] = hi
            WTl[1, s, at, k0:k1] = lo
            return 0

        lax.fori_loop(0, 8, step, 0)

    half_k = KD // 2
    loc[0].wait()
    transpose_in(0, 512)
    loc[1].wait()
    transpose_in(512, 1024)
    w0 = [swap_w(0, 0, 512)]
    loc[5].wait()
    d_zl.wait_recv()
    dx = Gather4(lambda h: DS.at[y, x, h], lambda i, h: DS.at[y, i, h], x, xi1, xi3, "x1", "x3")
    loc[2].wait()
    transpose_in(1024, 1536)
    w0.append(swap_w(0, 512, 1024))
    dx.forward()
    fx = Gather4(lambda h: ft.at[h * half_k:(h + 1) * half_k],
                 lambda i, h: FT.at[i, h * half_k:(h + 1) * half_k], x, xi1, xi3, "x1", "x3")
    loc[3].wait()
    loc[4].wait()
    transpose_in(1536, KP)
    w0.append(swap_w(0, 1024, 1536))
    loc[6].wait()
    dx.near()
    dx.far()
    w0.append(swap_w(0, 1536, KP))
    dy = Gather4(lambda h: DS.at[y, 2 * h:2 * h + 2], lambda i, h: DS.at[i, 2 * h:2 * h + 2],
                 y, yi1, yi3, "y1", "y3")
    w1 = [swap_w(1, 256 * j, 256 * j + 256) for j in range(4)]

    def convert(i):
        def step(j, _):
            k = pl.multiple_of(j * 64, 64)
            hi, lo = split(FT[i, pl.ds(k, 64), :])
            FTh[i, pl.ds(k, 64), :] = hi
            FTl[i, pl.ds(k, 64), :] = lo
            return 0

        lax.fori_loop(0, KD // 64, step, 0)
        a = lax.broadcasted_iota(jnp.int32, (64, 256), 0)
        b = lax.broadcasted_iota(jnp.int32, (64, 256), 1)
        mine = jnp.where(jnp.logical_and(i == y, zl == z1), 1, 0)
        e = jnp.where(b == a + (2 * z0 + core) * 64, mine, 0).astype(F32)
        FTh[i, KD:KP, :] = (-e).astype(BF16)
        FTl[i, KD:KP, :] = jnp.zeros((64, 256), BF16)

    def product(h, i, m, k0, k1, s_all, add):
        cols = pl.ds(pl.multiple_of(m * 256, 256), 256)

        def step(s, _):
            t = mm3(WTh[h, s, :, k0:k1], WTl[h, s, :, k0:k1], FTh[i, k0:k1], FTl[i, k0:k1], ((1,), (0,)))
            t = t.reshape(2, 2, 2, 2, 2, 8, 256)
            at = (s, h) + (slice(None),) * 6 + (cols,)
            PT[at] = PT[at] + t if add else t
            return 0

        lax.fori_loop(s_all[0], s_all[-1] + 1, step, 0)

    def product_all(h, k0, k1, s_all, add):
        def one(i, _):
            product(h, i, i, k0, k1, s_all, add)
            return 0

        lax.fori_loop(0, 4, one, 0)

    u1, u2 = (y0 + y1) % 2, y1
    v1, v2 = (z0 + z1) % 2, z1

    def al(v, n):
        return pl.multiple_of(v, n)

    LA, LB_ = slice(0, 512), slice(512, 1024)
    every = slice(None)

    def reduce_to_owner(s, h):
        d = go(PT.at[s, h, coreo], RC.at[s, h], "core")
        yield
        d.wait_recv()
        for i in range(2):
            PT[s, h, core, i] = PT[s, h, core, i] + RC[s, h, i]

        def swap(buf, a_to, a_send, a_keep, b_to, b_send, b_keep):
            def part(i, lanes):
                return (s, h, core) + i + (every,) * (5 - len(i)) + (lanes,)

            da = go(PT.at[part(a_send, LA)], buf.at[s, h, 0], a_to)
            db = go(PT.at[part(b_send, LB_)], buf.at[s, h, 1], b_to)
            yield
            for d_, keep, lanes, i in ((da, a_keep, LA, 0), (db, b_keep, LB_, 1)):
                d_.wait_recv()
                at = part(keep, lanes)
                PT[at] = PT[at] + buf[s, h, i]

        def full(*idx):
            return idx

        yield from swap(RYa, "y1", full(1 - u1), full(u1), "y3", full(every, 1 - u2), full(every, u2))
        yield from swap(RYb, "y3", full(u1, 1 - u2), full(u1, u2), "y1", full(1 - u1, u2), full(u1, u2))
        yield from swap(RZa, "z1", full(u1, u2, 1 - v1), full(u1, u2, v1),
                        "z3", full(u1, u2, every, 1 - v2), full(u1, u2, every, v2))
        yield from swap(RZb, "z3", full(u1, u2, v1, 1 - v2), full(u1, u2, v1, v2),
                        "z1", full(u1, u2, 1 - v1, v2), full(u1, u2, v1, v2))

    code = ((zl + z1) % 2) * 4 + ((x1 + y1) % 2) * 2 + (x0 + x1 + y0 + y1) % 2
    y2 = 2 * z0 + core
    last = []

    def spread(s):
        base = nsem[0]
        nsem[0] += 12

        def cp(p, t, from_wa):
            at = pl.ds(2 * (t % 2), 2)
            piece = LB.at[s, t // 2, at]
            return pltpu.make_async_remote_copy(
                src_ref=WA.at[s, t // 2, y2, at] if from_wa else piece, dst_ref=piece,
                send_sem=ssem.at[base + 4 * ("x1", "x3", "zl").index(p) + t],
                recv_sem=rsem.at[base + t], device_id=dev[p], device_id_type=MESH)

        @pl.when(code == 0)
        def _():
            for a, b, zz in ((0, 2, 0), (1, 3, 2), (2, 0, 1), (3, 1, 3)):
                cp("x1", a, True).start()
                cp("x3", b, True).start()
                cp("zl", zz, True).start()
            for t in range(2):
                for q in range(4):
                    LB[s, t, q] = WA[s, t, y2, q]

        roles = {1: ((0, 1, 2, 3), {0: "x3", 1: "x3"}), 2: ((2, 3, 0, 1), {2: "x1", 3: "x1"}),
                 3: ((0, 2, 1, 3), {})}
        for n in range(4):
            yield
            for k, (order, onward) in roles.items():
                @pl.when(code == k)
                def _(order=order, onward=onward):
                    t = order[n]
                    cp("zl", t, False).wait_recv()
                    if t in onward:
                        cp(onward[t], t, False).start()
                    cp("zl", t, False).start()

            @pl.when(code >= 4)
            def _():
                cp("zl", (0, 2, 1, 3)[n], False).wait_recv()

        def finish():
            @pl.when(code == 0)
            def _():
                for p in ("x1", "x3", "zl"):
                    for t in range(4):
                        cp(p, t, True).wait_send()

            for k, (order, onward) in roles.items():
                @pl.when(code == k)
                def _(onward=onward):
                    for t in range(4):
                        if t in onward:
                            cp(onward[t], t, False).wait_send()
                        cp("zl", t, False).wait_send()

        last.append(finish)

    def stream(s):
        yield from reduce_to_owner(s, 1)
        d = go(PT.at[s, 1, core, u1, u2, v1, v2], RG.at[s, zl, core, v1, v2], "zl")
        RG[s, zl, core, v1, v2] = PT[s, 0, core, u1, u2, v1, v2]
        yield
        d.wait_recv()

        def widen(*moves):
            ds_ = [go(RG.at[(s, every, core) + i + (every, lanes)],
                      RG.at[(s, every, core) + i + (every, lanes)], p) for i, lanes, p in moves]
            yield
            for d_ in ds_:
                d_.wait_recv()

        yield from widen(((v1, v2), LA, "z3"), ((v1, v2), LB_, "z1"))
        yield from widen(((v1, every), LA, "z1"), ((every, v2), LB_, "z3"))
        d = go(RG.at[s, :, core], RG.at[s, :, core], "core")
        yield
        d.wait_recv()
        acc = None
        for j in range(2):
            rh, rl = split(RG[s, j].reshape(64, 1024))
            lanes = pl.ds(j * 1024, 1024)
            t = mm3(rh, rl, DSh[0, :, lanes], DSh[1, :, lanes], ((1,), (1,)))
            acc = t if acc is None else acc + t
        WA[s, core, y, zh] = -acc

        wz = Gather4(lambda h: WA.at[s, core, y, zh, 32 * h:32 * h + 32],
                     lambda i, h: WA.at[s, core, y, i, 32 * h:32 * h + 32], zh, zi1, zi3, "z1", "z3")
        yield
        wz.forward()
        yield
        wz.near()
        wz.far()
        wy = Gather4(lambda h: WA.at[s, core, y, 2 * h:2 * h + 2],
                     lambda i, h: WA.at[s, core, i, 2 * h:2 * h + 2], y, yi1, yi3, "y1", "y3")
        wc = [go(WA.at[s, core, y], WA.at[s, core, y], "core")]
        yield
        wy.forward()
        yield
        wy.near()
        for i in (yi1, yi3):
            wc.append(go(WA.at[s, core, i], WA.at[s, core, i], "core"))
        yield
        wy.far()
        wc.append(go(WA.at[s, core, yi2], WA.at[s, core, yi2], "core"))
        yield
        for d in wc:
            d.wait_recv()
        yield from spread(s)

    def advance(*gens):
        for i in gens:
            next(i)

    def dsplit(q, _):
        for j in range(8):
            hi, lo = split(DS[q, j // 2, j % 2])
            lanes = pl.ds((j % 2) * 1024 + (j // 2) * 256, 256)
            DSh[0, pl.ds(al(q * 64, 64), 64), lanes] = hi
            DSh[1, pl.ds(al(q * 64, 64), 64), lanes] = lo
        return 0

    def more():
        k = 256 * len(w1)
        w1.append(swap_w(1, k, k + 256))

    both = (0, 1)
    convert(x)
    product(0, x, x, 0, KP, both, False)
    dy.forward()
    fx.forward()
    fx.near()
    more()
    for i in (xi1, xi3):
        convert(i)
        product(0, i, i, 0, KP, both, False)
    for d in w0:
        d.wait_recv()
    split_in(0, 0, KP)
    for i in (x, xi1, xi3):
        product(1, i, i, 0, KP, (0,), False)
    dy.near()
    dy.far()
    lax.fori_loop(0, 4, dsplit, 0)
    more()
    fx.far()
    convert(xi2)
    for h in range(2):
        product(h, xi2, xi2, 0, KP, (0,), False)
    early0, stream0 = reduce_to_owner(0, 0), stream(0)
    advance(early0, stream0)
    product(0, xi2, xi2, 0, KP, (1,), False)
    early1 = reduce_to_owner(1, 0)
    advance(early1)
    more()
    advance(early0, stream0)
    for j in range(4):
        w1[j].wait_recv()
    split_in(1, 0, 1024)
    product_all(1, 0, 1024, (1,), False)
    more()
    advance(early0, stream0, early1)
    for j in range(4, 6):
        w1[j].wait_recv()
    split_in(1, 1024, 1536)
    product_all(1, 1024, 1536, (1,), True)
    advance(early0, stream0, early1)
    for j in range(6, 8):
        w1[j].wait_recv()
        split_in(1, 256 * j, 256 * j + 256)
        product_all(1, 256 * j, 256 * j + 256, (1,), True)
    pending = [early0, stream0, early1, stream(1)]
    next(pending[-1])
    while pending:
        for i in list(pending):
            if next(i, "end") == "end":
                pending.remove(i)

    for q in range(4):
        blk = pl.ds(al(y1 * 128, 128), 128)
        TW[q] = jnp.concatenate([WA[0, core, q, zh, :, blk], WA[1, core, q, zh, :, blk]], axis=0).T
        w_out[:, q * 128:(q + 1) * 128] = TW[q, pl.ds(al(y0 * 64, 64), 64), :]

    gram_out[...] = jnp.zeros_like(gram_out)

    def gram_step(i, _):
        a, b = i // 4, i % 4
        lh, ll = split(jnp.concatenate([LB[0, a, b], LB[1, a, b]], axis=0))
        rh, rl = split(jnp.concatenate([WA[s, a, q, b] for q in range(4) for s in range(2)], axis=0))
        gram_out[...] = gram_out[...] + mm3(lh, ll, rh, rl, ((1,), (1,)))
        return 0

    lax.fori_loop(0, 8, gram_step, 0)
    gram_out[...] = gram_out[...] * (1.0 / ROWS)
    for d in sends:
        d.wait_send()
    for end in last:
        end()
    assert nsem[0] <= NSEM


def body(f, wb, g, di):
    ft = f.T
    vm, dma = pltpu.VMEM, pltpu.SemaphoreType.DMA
    return pl.pallas_call(
        kernel,
        out_shape=(jax.ShapeDtypeStruct((64, 512), F32), jax.ShapeDtypeStruct((128, 512), F32)),
        in_specs=[pl.BlockSpec(memory_space=pl.ANY)] * 4,
        out_specs=(pl.BlockSpec(memory_space=pltpu.VMEM),) * 2,
        scratch_shapes=[
            vm((4, KD, 256), F32), vm((4, KP, 256), BF16), vm((4, KP, 256), BF16),
            vm((KP, 512), F32), vm((2, 256, KP), F32), vm((2, 256, KP), F32),
            vm((2, 2, 256, KP), BF16), vm((2, 2, 256, KP), BF16),
            vm((2, 2, 2, 2, 2, 2, 2, 8, 1024), F32), vm((2, 2, 2, 2, 2, 2, 8, 1024), F32),
            vm((2, 2, 2, 2, 2, 2, 8, 512), F32), vm((2, 2, 2, 2, 2, 8, 512), F32),
            vm((2, 2, 2, 2, 8, 512), F32), vm((2, 2, 2, 8, 512), F32),
            vm((2, 2, 2, 2, 2, 8, 1024), F32), vm((4, 4, 2, 64, 256), F32), vm((2, 256, 2048), BF16),
            vm((2, 2, 4, 4, 64, 256), F32), vm((2, 2, 4, 64, 256), F32), vm((4, 128, 128), F32),
            dma((NSEM,)), dma((NSEM,)), dma((10,)),
        ],
        compiler_params=pltpu.CompilerParams(collective_id=0, has_side_effects=True,
                                             vmem_limit_bytes=66_000_000),
        name="panel",
    )(ft, wb, g, di)


def solution(mesh):
    return jax.shard_map(
        body, mesh=mesh,
        in_specs=(P("pcol", "prow"), P("prow", "pcol"), P("prow", "pcol"), P("prow", "pcol")),
        out_specs=(P("prow", "pcol"), P("prow", "pcol")), check_vma=False)
```

```python
import jax
import jax.numpy as jnp
from jax import lax
from jax.experimental import pallas as pl
from jax.experimental.pallas import tpu as pltpu
from jax.sharding import PartitionSpec as P

F32 = jnp.float32
BF16 = jnp.bfloat16
MESH = pl.DeviceIdType.MESH
ROWS = 2048
KD = 1984
KP = 2048
NSEM = 140
CUTS = (0, 512, 1024, 1536, KD)


def split(v):
    hi = v.astype(BF16)
    return hi, (v - hi.astype(F32)).astype(BF16)


def mm(a, b, dims):
    return lax.dot_general(a, b, (dims, ((), ())), preferred_element_type=F32)


def mm3(ah, al, bh, bl, dims):
    return mm(ah, bh, dims) + (mm(ah, bl, dims) + mm(al, bh, dims))


def kernel(ft, wb, g, di, w_out, gram_out, FT, FTh, FTl, WB, OT, IT, WTh, WTl, PT, RC, RYa, RYb,
           RZa, RZb, RG, DS, DSh, WA, LB, TW, ssem, rsem, lsem):
    r = lax.axis_index("prow")
    c = lax.axis_index("pcol")
    core = r % 2
    z0, z1 = (r // 2) % 2, (r // 4) % 2
    y0, y1 = (r // 8) % 2, r // 16
    zl = c % 2
    x0, x1 = (c // 2) % 2, c // 4
    zh, y, x = z0 + 2 * z1, y0 + 2 * y1, x0 + 2 * x1

    def near(b0, b1, base, unit):
        p1 = base + unit * (1 - 2 * b0)
        return p1, p1 + 2 * unit * (1 - 2 * b1), base + 2 * unit * (1 - 2 * b1)

    r_core = r + 1 - 2 * core
    r_z1, r_z3, _ = near(z0, z1, r, 2)
    r_y1, r_y3, _ = near(y0, y1, r, 8)
    c_zl = c + 1 - 2 * zl
    c_x1, c_x3, _ = near(x0, x1, c, 2)
    zi1, zi3, zi2 = near(z0, z1, zh, 1)
    yi1, yi3, yi2 = near(y0, y1, y, 1)
    xi1, xi3, xi2 = near(x0, x1, x, 1)
    zlo = 1 - zl
    coreo = 1 - core
    dev = {"core": (r_core, c), "z1": (r_z1, c), "z3": (r_z3, c), "y1": (r_y1, c), "y3": (r_y3, c),
           "zl": (r, c_zl), "x1": (r, c_x1), "x3": (r, c_x3)}

    nsem = [0]
    sends = []

    def rc(src, dst, peer, rs=None, keep=True):
        i = nsem[0]
        nsem[0] += 1
        d = pltpu.make_async_remote_copy(src_ref=src, dst_ref=dst, send_sem=ssem.at[i],
                                         recv_sem=rsem.at[i if rs is None else rs],
                                         device_id=dev[peer], device_id_type=MESH)
        if keep:
            sends.append(d)
        return d

    def go(*a):
        d = rc(*a)
        d.start()
        return d

    bar = pltpu.get_barrier_semaphore()
    for p in dev.values():
        pl.semaphore_signal(bar, inc=1, device_id=p, device_id_type=MESH)
    pl.semaphore_wait(bar, len(dev))

    class Gather4:
        def __init__(self, own, slot, me, i1, i3, p1, p3):
            self.slot, self.i, self.p = slot, (me, i1, i3), (p1, p3)
            self.c1 = go(own(0), slot(me, 0), p1)
            self.c2 = go(own(1), slot(me, 1), p3)
            self.c3 = go(own(1), slot(me, 1), p1)
            self.c4 = go(own(0), slot(me, 0), p3)

        def forward(self):
            (_, i1, i3), (p1, p3) = self.i, self.p
            self.c1.wait_recv()
            self.f1 = go(self.slot(i1, 0), self.slot(i1, 0), p3)
            self.c2.wait_recv()
            self.f2 = go(self.slot(i3, 1), self.slot(i3, 1), p1)

        def near(self):
            self.c3.wait_recv()
            self.c4.wait_recv()

        def far(self):
            self.f1.wait_recv()
            self.f2.wait_recv()

    d_zl = go(di, DS.at[y, x, zl], "zl")
    loc = []

    def lc(src, dst):
        d = pltpu.make_async_copy(src, dst, lsem.at[len(loc)])
        d.start()
        loc.append(d)

    for a, b in zip(CUTS[:-1], CUTS[1:]):
        lc(wb.at[a:b], WB.at[a:b])
    lc(g, WB.at[KD:KP])
    lc(di, DS.at[y, x, zl])
    lc(ft, FT.at[x])

    def transpose_in(k0, k1):
        def step(i, _):
            k = pl.multiple_of(i * 256, 256)
            at = pl.ds(k, 256)
            for q in range(4):
                qi = 2 * ((q % 2 + q // 2) % 2) + q // 2
                v = WB[at, q * 128:(q + 1) * 128].T
                hi, lo = split(v)
                for s in range(2):
                    for ck in range(2):
                        f = slice(s * 64 + ck * 32, s * 64 + ck * 32 + 32)
                        t = slice(ck * 128 + qi * 32, ck * 128 + qi * 32 + 32)
                        OT[s, t, at] = v[f]
                        WTh[0, s, t, at] = hi[f]
                        WTl[0, s, t, at] = lo[f]
            return 0

        lax.fori_loop(k0 // 256, k1 // 256, step, 0)

    def swap_w(s, k0, k1):
        return go(OT.at[s, :, k0:k1], IT.at[s, :, k0:k1], "zl")

    def split_in(s, k0, k1):
        def step(i, _):
            at = pl.ds(pl.multiple_of(i * 32, 32), 32)
            hi, lo = split(IT[s, at, k0:k1])
            WTh[1, s, at, k0:k1] = hi
            WTl[1, s, at, k0:k1] = lo
            return 0

        lax.fori_loop(0, 8, step, 0)

    half_k = KD // 2
    loc[0].wait()
    transpose_in(0, 512)
    loc[1].wait()
    transpose_in(512, 1024)
    w0 = [swap_w(0, 0, 512)]
    loc[5].wait()
    d_zl.wait_recv()
    dx = Gather4(lambda h: DS.at[y, x, h], lambda i, h: DS.at[y, i, h], x, xi1, xi3, "x1", "x3")
    loc[2].wait()
    transpose_in(1024, 1536)
    w0.append(swap_w(0, 512, 1024))
    dx.forward()
    fx = Gather4(lambda h: ft.at[h * half_k:(h + 1) * half_k],
                 lambda i, h: FT.at[i, h * half_k:(h + 1) * half_k], x, xi1, xi3, "x1", "x3")
    loc[3].wait()
    loc[4].wait()
    transpose_in(1536, KP)
    w0.append(swap_w(0, 1024, 1536))
    loc[6].wait()
    dx.near()
    dx.far()
    w0.append(swap_w(0, 1536, KP))
    dy = Gather4(lambda h: DS.at[y, 2 * h:2 * h + 2], lambda i, h: DS.at[i, 2 * h:2 * h + 2],
                 y, yi1, yi3, "y1", "y3")
    w1 = [swap_w(1, 256 * j, 256 * j + 256) for j in range(4)]

    def convert(i):
        def step(j, _):
            k = pl.multiple_of(j * 64, 64)
            hi, lo = split(FT[i, pl.ds(k, 64), :])
            FTh[i, pl.ds(k, 64), :] = hi
            FTl[i, pl.ds(k, 64), :] = lo
            return 0

        lax.fori_loop(0, KD // 64, step, 0)
        a = lax.broadcasted_iota(jnp.int32, (64, 256), 0)
        b = lax.broadcasted_iota(jnp.int32, (64, 256), 1)
        mine = jnp.where(jnp.logical_and(i == y, zl == z1), 1, 0)
        e = jnp.where(b == a + (2 * z0 + core) * 64, mine, 0).astype(F32)
        FTh[i, KD:KP, :] = (-e).astype(BF16)
        FTl[i, KD:KP, :] = jnp.zeros((64, 256), BF16)

    def product(h, i, m, k0, k1, s_all, add):
        cols = pl.ds(pl.multiple_of(m * 256, 256), 256)

        def step(s, _):
            t = mm3(WTh[h, s, :, k0:k1], WTl[h, s, :, k0:k1], FTh[i, k0:k1], FTl[i, k0:k1], ((1,), (0,)))
            t = t.reshape(2, 2, 2, 2, 2, 8, 256)
            at = (s, h) + (slice(None),) * 6 + (cols,)
            PT[at] = PT[at] + t if add else t
            return 0

        lax.fori_loop(s_all[0], s_all[-1] + 1, step, 0)

    def product_all(h, k0, k1, s_all, add):
        def one(i, _):
            product(h, i, i, k0, k1, s_all, add)
            return 0

        lax.fori_loop(0, 4, one, 0)

    u1, u2 = (y0 + y1) % 2, y1
    v1, v2 = (z0 + z1) % 2, z1

    def al(v, n):
        return pl.multiple_of(v, n)

    LA, LB_ = slice(0, 512), slice(512, 1024)
    every = slice(None)

    def reduce_to_owner(s, h):
        d = go(PT.at[s, h, coreo], RC.at[s, h], "core")
        yield
        d.wait_recv()
        for i in range(2):
            PT[s, h, core, i] = PT[s, h, core, i] + RC[s, h, i]

        def swap(buf, a_to, a_send, a_keep, b_to, b_send, b_keep):
            def part(i, lanes):
                return (s, h, core) + i + (every,) * (5 - len(i)) + (lanes,)

            da = go(PT.at[part(a_send, LA)], buf.at[s, h, 0], a_to)
            db = go(PT.at[part(b_send, LB_)], buf.at[s, h, 1], b_to)
            yield
            for d_, keep, lanes, i in ((da, a_keep, LA, 0), (db, b_keep, LB_, 1)):
                d_.wait_recv()
                at = part(keep, lanes)
                PT[at] = PT[at] + buf[s, h, i]

        def full(*idx):
            return idx

        yield from swap(RYa, "y1", full(1 - u1), full(u1), "y3", full(every, 1 - u2), full(every, u2))
        yield from swap(RYb, "y3", full(u1, 1 - u2), full(u1, u2), "y1", full(1 - u1, u2), full(u1, u2))
        yield from swap(RZa, "z1", full(u1, u2, 1 - v1), full(u1, u2, v1),
                        "z3", full(u1, u2, every, 1 - v2), full(u1, u2, every, v2))
        yield from swap(RZb, "z3", full(u1, u2, v1, 1 - v2), full(u1, u2, v1, v2),
                        "z1", full(u1, u2, 1 - v1, v2), full(u1, u2, v1, v2))

    code = ((zl + z1) % 2) * 4 + ((x1 + y1) % 2) * 2 + (x0 + x1 + y0 + y1) % 2
    y2 = 2 * z0 + core
    last = []
    arrived = []

    def own_block(i0, i1):
        def step(i, _):
            a, b = i // 4, i % 4
            at = pl.ds(al(i * 256, 256), 256)
            for q in range(4):
                for s in range(2):
                    f = (q % 2) * 128 + s * 64
                    hi, lo = split(WA[s, a, q, b])
                    WTh[0, q // 2, f:f + 64, at] = hi
                    WTl[0, q // 2, f:f + 64, at] = lo
            return 0

        lax.fori_loop(i0, i1, step, 0)

    def gram(s):
        lh, ll = split(jnp.concatenate([LB[s, i // 4, i % 4] for i in range(8)], axis=1))
        for j in range(2):
            gram_out[s * 64:s * 64 + 64, j * 256:j * 256 + 256] = mm3(
                lh, ll, WTh[0, j], WTl[0, j], ((1,), (1,)))

    def beside(n):
        if n == 0:
            own_block(0, 4)
            for q in range(4):
                blk = pl.ds(al(y1 * 128, 128), 128)
                TW[q] = jnp.concatenate([WA[0, core, q, zh, :, blk], WA[1, core, q, zh, :, blk]], axis=0).T
                w_out[:, q * 128:(q + 1) * 128] = TW[q, pl.ds(al(y0 * 64, 64), 64), :]
        elif n == 1:
            own_block(4, 8)
        elif n == 2:
            assert arrived
            gram(0)

    def spread(s, beside=None):
        base = nsem[0]
        nsem[0] += 12

        def cp(p, t, from_wa):
            at = pl.ds(2 * (t % 2), 2)
            piece = LB.at[s, t // 2, at]
            return pltpu.make_async_remote_copy(
                src_ref=WA.at[s, t // 2, y2, at] if from_wa else piece, dst_ref=piece,
                send_sem=ssem.at[base + 4 * ("x1", "x3", "zl").index(p) + t],
                recv_sem=rsem.at[base + t], device_id=dev[p], device_id_type=MESH)

        @pl.when(code == 0)
        def _():
            for a, b, zz in ((0, 2, 0), (1, 3, 2), (2, 0, 1), (3, 1, 3)):
                cp("x1", a, True).start()
                cp("x3", b, True).start()
                cp("zl", zz, True).start()
            for t in range(2):
                for q in range(4):
                    LB[s, t, q] = WA[s, t, y2, q]

        roles = {1: ((0, 1, 2, 3), {0: "x3", 1: "x3"}), 2: ((2, 3, 0, 1), {2: "x1", 3: "x1"}),
                 3: ((0, 2, 1, 3), {})}
        for n in range(4):
            yield
            for k, (order, onward) in roles.items():
                @pl.when(code == k)
                def _(order=order, onward=onward):
                    t = order[n]
                    cp("zl", t, False).wait_recv()
                    if t in onward:
                        cp(onward[t], t, False).start()
                    cp("zl", t, False).start()

            @pl.when(code >= 4)
            def _():
                cp("zl", (0, 2, 1, 3)[n], False).wait_recv()

            if beside is not None:
                beside(n)
            elif n == 3:
                arrived.append(s)

        def finish():
            @pl.when(code == 0)
            def _():
                for p in ("x1", "x3", "zl"):
                    for t in range(4):
                        cp(p, t, True).wait_send()

            for k, (order, onward) in roles.items():
                @pl.when(code == k)
                def _(onward=onward):
                    for t in range(4):
                        if t in onward:
                            cp(onward[t], t, False).wait_send()
                        cp("zl", t, False).wait_send()

        last.append(finish)

    def stream(s):
        yield from reduce_to_owner(s, 1)
        d = go(PT.at[s, 1, core, u1, u2, v1, v2], RG.at[s, zl, core, v1, v2], "zl")
        RG[s, zl, core, v1, v2] = PT[s, 0, core, u1, u2, v1, v2]
        yield
        d.wait_recv()

        def widen(*moves):
            ds_ = [go(RG.at[(s, every, core) + i + (every, lanes)],
                      RG.at[(s, every, core) + i + (every, lanes)], p) for i, lanes, p in moves]
            yield
            for d_ in ds_:
                d_.wait_recv()

        yield from widen(((v1, v2), LA, "z3"), ((v1, v2), LB_, "z1"))
        yield from widen(((v1, every), LA, "z1"), ((every, v2), LB_, "z3"))
        d = go(RG.at[s, :, core], RG.at[s, :, core], "core")
        yield
        d.wait_recv()
        acc = None
        for j in range(2):
            rh, rl = split(RG[s, j].reshape(64, 1024))
            lanes = pl.ds(j * 1024, 1024)
            t = mm3(rh, rl, DSh[0, :, lanes], DSh[1, :, lanes], ((1,), (1,)))
            acc = t if acc is None else acc + t
        WA[s, core, y, zh] = acc

        wz = Gather4(lambda h: WA.at[s, core, y, zh, 32 * h:32 * h + 32],
                     lambda i, h: WA.at[s, core, y, i, 32 * h:32 * h + 32], zh, zi1, zi3, "z1", "z3")
        yield
        wz.forward()
        yield
        wz.near()
        wz.far()
        wy = Gather4(lambda h: WA.at[s, core, y, 2 * h:2 * h + 2],
                     lambda i, h: WA.at[s, core, i, 2 * h:2 * h + 2], y, yi1, yi3, "y1", "y3")
        wc = [go(WA.at[s, core, y], WA.at[s, core, y], "core")]
        yield
        wy.forward()
        yield
        wy.near()
        for i in (yi1, yi3):
            wc.append(go(WA.at[s, core, i], WA.at[s, core, i], "core"))
        yield
        wy.far()
        wc.append(go(WA.at[s, core, yi2], WA.at[s, core, yi2], "core"))
        yield
        for d in wc:
            d.wait_recv()
        yield from spread(s, (None, beside)[s])

    def advance(*gens):
        for i in gens:
            next(i)

    def dsplit(q, _):
        for j in range(8):
            hi, lo = split(DS[q, j // 2, j % 2])
            lanes = pl.ds((j % 2) * 1024 + (j // 2) * 256, 256)
            DSh[0, pl.ds(al(q * 64, 64), 64), lanes] = hi
            DSh[1, pl.ds(al(q * 64, 64), 64), lanes] = lo
        return 0

    def more():
        k = 256 * len(w1)
        w1.append(swap_w(1, k, k + 256))

    both = (0, 1)
    convert(x)
    product(0, x, x, 0, KP, both, False)
    dy.forward()
    fx.forward()
    fx.near()
    more()
    for i in (xi1, xi3):
        convert(i)
        product(0, i, i, 0, KP, both, False)
    for d in w0:
        d.wait_recv()
    split_in(0, 0, KP)
    for i in (x, xi1, xi3):
        product(1, i, i, 0, KP, (0,), False)
    dy.near()
    dy.far()
    lax.fori_loop(0, 4, dsplit, 0)
    more()
    more()
    fx.far()
    convert(xi2)
    for h in range(2):
        product(h, xi2, xi2, 0, KP, (0,), False)
    early0, stream0 = reduce_to_owner(0, 0), stream(0)
    advance(early0, stream0)
    product(0, xi2, xi2, 0, KP, (1,), False)
    early1 = reduce_to_owner(1, 0)
    advance(early1)
    more()
    advance(early0, stream0)
    for j in range(4):
        w1[j].wait_recv()
    split_in(1, 0, 1024)
    product_all(1, 0, 1024, (1,), False)
    advance(early0, stream0, early1)
    for j in range(4, 6):
        w1[j].wait_recv()
    split_in(1, 1024, 1536)
    product_all(1, 1024, 1536, (1,), True)
    advance(early0, stream0, early1)
    for j in range(6, 8):
        w1[j].wait_recv()
        split_in(1, 256 * j, 256 * j + 256)
        product_all(1, 256 * j, 256 * j + 256, (1,), True)
    pending = [early0, stream0, early1, stream(1)]
    next(pending[-1])
    while pending:
        for i in list(pending):
            if next(i, "end") == "end":
                pending.remove(i)

    gram(1)
    for d in sends:
        d.wait_send()
    for end in last:
        end()
    assert nsem[0] <= NSEM


def body(f, wb, g, di):
    ft = f.T
    vm, dma = pltpu.VMEM, pltpu.SemaphoreType.DMA
    w, gram = pl.pallas_call(
        kernel,
        out_shape=(jax.ShapeDtypeStruct((64, 512), F32), jax.ShapeDtypeStruct((128, 512), F32)),
        in_specs=[pl.BlockSpec(memory_space=pl.ANY)] * 4,
        out_specs=(pl.BlockSpec(memory_space=pltpu.VMEM),) * 2,
        scratch_shapes=[
            vm((4, KD, 256), F32), vm((4, KP, 256), BF16), vm((4, KP, 256), BF16),
            vm((KP, 512), F32), vm((2, 256, KP), F32), vm((2, 256, KP), F32),
            vm((2, 2, 256, KP), BF16), vm((2, 2, 256, KP), BF16),
            vm((2, 2, 2, 2, 2, 2, 2, 8, 1024), F32), vm((2, 2, 2, 2, 2, 2, 8, 1024), F32),
            vm((2, 2, 2, 2, 2, 2, 8, 512), F32), vm((2, 2, 2, 2, 2, 8, 512), F32),
            vm((2, 2, 2, 2, 8, 512), F32), vm((2, 2, 2, 8, 512), F32),
            vm((2, 2, 2, 2, 2, 8, 1024), F32), vm((4, 4, 2, 64, 256), F32), vm((2, 256, 2048), BF16),
            vm((2, 2, 4, 4, 64, 256), F32), vm((2, 2, 4, 64, 256), F32), vm((4, 128, 128), F32),
            dma((NSEM,)), dma((NSEM,)), dma((10,)),
        ],
        compiler_params=pltpu.CompilerParams(collective_id=0, has_side_effects=True,
                                             vmem_limit_bytes=66_000_000),
        name="panel",
    )(ft, wb, g, di)
    return -w, gram * (1.0 / ROWS)


def solution(mesh):
    return jax.shard_map(
        body, mesh=mesh,
        in_specs=(P("pcol", "prow"), P("prow", "pcol"), P("prow", "pcol"), P("prow", "pcol")),
        out_specs=(P("prow", "pcol"), P("prow", "pcol")), check_vma=False)
```

```python
import jax
import jax.numpy as jnp
from jax import lax
from jax.experimental import pallas as pl
from jax.experimental.pallas import tpu as pltpu
from jax.sharding import PartitionSpec as P

F32 = jnp.float32
BF16 = jnp.bfloat16
MESH = pl.DeviceIdType.MESH
ROWS = 2048
KD = 1984
KP = 2048
NSEM = 140
CUTS = (0, 512, 1024, 1536, KD)


def split(v):
    hi = v.astype(BF16)
    return hi, (v - hi.astype(F32)).astype(BF16)


def mm(a, b, dims):
    return lax.dot_general(a, b, (dims, ((), ())), preferred_element_type=F32)


def mm3(ah, al, bh, bl, dims):
    return mm(ah, bh, dims) + (mm(ah, bl, dims) + mm(al, bh, dims))


def kernel(ft, wb, g, di, w_out, gram_out, FT, FTh, FTl, WB, OT, IT, WTh, WTl, PT, RC, RYa, RYb,
           RZa, RZb, RG, DS, DSh, WA, LB, TW, ssem, rsem, lsem):
    r = lax.axis_index("prow")
    c = lax.axis_index("pcol")
    core = r % 2
    z0, z1 = (r // 2) % 2, (r // 4) % 2
    y0, y1 = (r // 8) % 2, r // 16
    zl = c % 2
    x0, x1 = (c // 2) % 2, c // 4
    zh, y, x = z0 + 2 * z1, y0 + 2 * y1, x0 + 2 * x1

    def near(b0, b1, base, unit):
        p1 = base + unit * (1 - 2 * b0)
        return p1, p1 + 2 * unit * (1 - 2 * b1), base + 2 * unit * (1 - 2 * b1)

    r_core = r + 1 - 2 * core
    r_z1, r_z3, _ = near(z0, z1, r, 2)
    r_y1, r_y3, _ = near(y0, y1, r, 8)
    c_zl = c + 1 - 2 * zl
    c_x1, c_x3, _ = near(x0, x1, c, 2)
    zi1, zi3, zi2 = near(z0, z1, zh, 1)
    yi1, yi3, yi2 = near(y0, y1, y, 1)
    xi1, xi3, xi2 = near(x0, x1, x, 1)
    zlo = 1 - zl
    coreo = 1 - core
    dev = {"core": (r_core, c), "z1": (r_z1, c), "z3": (r_z3, c), "y1": (r_y1, c), "y3": (r_y3, c),
           "zl": (r, c_zl), "x1": (r, c_x1), "x3": (r, c_x3)}

    nsem = [0]
    sends = []

    def rc(src, dst, peer, rs=None, keep=True):
        i = nsem[0]
        nsem[0] += 1
        d = pltpu.make_async_remote_copy(src_ref=src, dst_ref=dst, send_sem=ssem.at[i],
                                         recv_sem=rsem.at[i if rs is None else rs],
                                         device_id=dev[peer], device_id_type=MESH)
        if keep:
            sends.append(d)
        return d

    def go(*a):
        d = rc(*a)
        d.start()
        return d

    bar = pltpu.get_barrier_semaphore()
    for p in dev.values():
        pl.semaphore_signal(bar, inc=1, device_id=p, device_id_type=MESH)
    pl.semaphore_wait(bar, len(dev))

    class Gather4:
        def __init__(self, own, slot, me, i1, i3, p1, p3):
            self.slot, self.i, self.p = slot, (me, i1, i3), (p1, p3)
            self.c1 = go(own(0), slot(me, 0), p1)
            self.c2 = go(own(1), slot(me, 1), p3)
            self.c3 = go(own(1), slot(me, 1), p1)
            self.c4 = go(own(0), slot(me, 0), p3)

        def forward(self):
            (_, i1, i3), (p1, p3) = self.i, self.p
            self.c1.wait_recv()
            self.f1 = go(self.slot(i1, 0), self.slot(i1, 0), p3)
            self.c2.wait_recv()
            self.f2 = go(self.slot(i3, 1), self.slot(i3, 1), p1)

        def near(self):
            self.c3.wait_recv()
            self.c4.wait_recv()

        def far(self):
            self.f1.wait_recv()
            self.f2.wait_recv()

    d_zl = go(di, DS.at[y, x, zl], "zl")
    loc = []

    def lc(src, dst):
        d = pltpu.make_async_copy(src, dst, lsem.at[len(loc)])
        d.start()
        loc.append(d)

    for a, b in zip(CUTS[:-1], CUTS[1:]):
        lc(wb.at[a:b], WB.at[a:b])
    lc(g, WB.at[KD:KP])
    lc(di, DS.at[y, x, zl])
    lc(ft, FT.at[x])

    def transpose_in(k0, k1):
        def step(i, _):
            k = pl.multiple_of(i * 256, 256)
            at = pl.ds(k, 256)
            for q in range(4):
                qi = 2 * ((q % 2 + q // 2) % 2) + q // 2
                v = WB[at, q * 128:(q + 1) * 128].T
                hi, lo = split(v)
                for s in range(2):
                    for ck in range(2):
                        f = slice(s * 64 + ck * 32, s * 64 + ck * 32 + 32)
                        t = slice(ck * 128 + qi * 32, ck * 128 + qi * 32 + 32)
                        OT[s, t, at] = v[f]
                        WTh[0, s, t, at] = hi[f]
                        WTl[0, s, t, at] = lo[f]
            return 0

        lax.fori_loop(k0 // 256, k1 // 256, step, 0)

    def swap_w(s, k0, k1):
        return go(OT.at[s, :, k0:k1], IT.at[s, :, k0:k1], "zl")

    def split_in(s, k0, k1):
        def step(i, _):
            at = pl.ds(pl.multiple_of(i * 32, 32), 32)
            hi, lo = split(IT[s, at, k0:k1])
            WTh[1, s, at, k0:k1] = hi
            WTl[1, s, at, k0:k1] = lo
            return 0

        lax.fori_loop(0, 8, step, 0)

    half_k = KD // 2
    loc[0].wait()
    transpose_in(0, 256)
    transpose_in(256, 512)
    w0 = [swap_w(0, 0, 256)]
    loc[5].wait()
    d_zl.wait_recv()
    dx = Gather4(lambda h: DS.at[y, x, h], lambda i, h: DS.at[y, i, h], x, xi1, xi3, "x1", "x3")
    loc[1].wait()
    transpose_in(512, 1024)
    w0.append(swap_w(0, 256, 512))
    dx.forward()
    fx = Gather4(lambda h: ft.at[h * half_k:(h + 1) * half_k],
                 lambda i, h: FT.at[i, h * half_k:(h + 1) * half_k], x, xi1, xi3, "x1", "x3")
    loc[2].wait()
    transpose_in(1024, 1536)
    w0.append(swap_w(0, 512, 1024))
    loc[3].wait()
    loc[4].wait()
    transpose_in(1536, KP)
    w0.append(swap_w(0, 1024, 1536))
    loc[6].wait()
    dx.near()
    dx.far()
    w0.append(swap_w(0, 1536, KP))
    dy = Gather4(lambda h: DS.at[y, 2 * h:2 * h + 2], lambda i, h: DS.at[i, 2 * h:2 * h + 2],
                 y, yi1, yi3, "y1", "y3")
    w1 = [swap_w(1, 256 * j, 256 * j + 256) for j in range(4)]

    def convert(i):
        def step(j, _):
            k = pl.multiple_of(j * 64, 64)
            hi, lo = split(FT[i, pl.ds(k, 64), :])
            FTh[i, pl.ds(k, 64), :] = hi
            FTl[i, pl.ds(k, 64), :] = lo
            return 0

        lax.fori_loop(0, KD // 64, step, 0)
        a = lax.broadcasted_iota(jnp.int32, (64, 256), 0)
        b = lax.broadcasted_iota(jnp.int32, (64, 256), 1)
        mine = jnp.where(jnp.logical_and(i == y, zl == z1), 1, 0)
        e = jnp.where(b == a + (2 * z0 + core) * 64, mine, 0).astype(F32)
        FTh[i, KD:KP, :] = (-e).astype(BF16)
        FTl[i, KD:KP, :] = jnp.zeros((64, 256), BF16)

    def product(h, i, m, k0, k1, s_all, add):
        cols = pl.ds(pl.multiple_of(m * 256, 256), 256)

        def step(s, _):
            t = mm3(WTh[h, s, :, k0:k1], WTl[h, s, :, k0:k1], FTh[i, k0:k1], FTl[i, k0:k1], ((1,), (0,)))
            t = t.reshape(2, 2, 2, 2, 2, 8, 256)
            at = (s, h) + (slice(None),) * 6 + (cols,)
            PT[at] = PT[at] + t if add else t
            return 0

        lax.fori_loop(s_all[0], s_all[-1] + 1, step, 0)

    def product_all(h, k0, k1, s_all, add):
        def one(i, _):
            product(h, i, i, k0, k1, s_all, add)
            return 0

        lax.fori_loop(0, 4, one, 0)

    u1, u2 = (y0 + y1) % 2, y1
    v1, v2 = (z0 + z1) % 2, z1

    def al(v, n):
        return pl.multiple_of(v, n)

    LA, LB_ = slice(0, 512), slice(512, 1024)
    every = slice(None)

    def reduce_to_owner(s, h):
        d = go(PT.at[s, h, coreo], RC.at[s, h], "core")
        yield
        d.wait_recv()
        for i in range(2):
            PT[s, h, core, i] = PT[s, h, core, i] + RC[s, h, i]

        def swap(buf, a_to, a_send, a_keep, b_to, b_send, b_keep):
            def part(i, lanes):
                return (s, h, core) + i + (every,) * (5 - len(i)) + (lanes,)

            da = go(PT.at[part(a_send, LA)], buf.at[s, h, 0], a_to)
            db = go(PT.at[part(b_send, LB_)], buf.at[s, h, 1], b_to)
            yield
            for d_, keep, lanes, i in ((da, a_keep, LA, 0), (db, b_keep, LB_, 1)):
                d_.wait_recv()
                at = part(keep, lanes)
                PT[at] = PT[at] + buf[s, h, i]

        def full(*idx):
            return idx

        yield from swap(RYa, "y1", full(1 - u1), full(u1), "y3", full(every, 1 - u2), full(every, u2))
        yield from swap(RYb, "y3", full(u1, 1 - u2), full(u1, u2), "y1", full(1 - u1, u2), full(u1, u2))
        yield from swap(RZa, "z1", full(u1, u2, 1 - v1), full(u1, u2, v1),
                        "z3", full(u1, u2, every, 1 - v2), full(u1, u2, every, v2))
        yield from swap(RZb, "z3", full(u1, u2, v1, 1 - v2), full(u1, u2, v1, v2),
                        "z1", full(u1, u2, 1 - v1, v2), full(u1, u2, v1, v2))

    code = ((zl + z1) % 2) * 4 + ((x1 + y1) % 2) * 2 + (x0 + x1 + y0 + y1) % 2
    y2 = 2 * z0 + core
    last = []
    arrived = []

    def own_block(i0, i1):
        def step(i, _):
            a, b = i // 4, i % 4
            at = pl.ds(al(i * 256, 256), 256)
            for q in range(4):
                for s in range(2):
                    f = (q % 2) * 128 + s * 64
                    hi, lo = split(WA[s, a, q, b])
                    WTh[0, q // 2, f:f + 64, at] = hi
                    WTl[0, q // 2, f:f + 64, at] = lo
            return 0

        lax.fori_loop(i0, i1, step, 0)

    def gram(s):
        lh, ll = split(jnp.concatenate([LB[s, i // 4, i % 4] for i in range(8)], axis=1))
        for j in range(2):
            gram_out[s * 64:s * 64 + 64, j * 256:j * 256 + 256] = mm3(
                lh, ll, WTh[0, j], WTl[0, j], ((1,), (1,)))

    def beside(n):
        if n == 0:
            own_block(0, 4)
            for q in range(4):
                blk = pl.ds(al(y1 * 128, 128), 128)
                TW[q] = jnp.concatenate([WA[0, core, q, zh, :, blk], WA[1, core, q, zh, :, blk]], axis=0).T
                w_out[:, q * 128:(q + 1) * 128] = TW[q, pl.ds(al(y0 * 64, 64), 64), :]
        elif n == 1:
            own_block(4, 8)
        elif n == 2:
            assert arrived
            gram(0)

    def spread(s, beside=None):
        base = nsem[0]
        nsem[0] += 12

        def cp(p, t, from_wa):
            at = pl.ds(2 * (t % 2), 2)
            piece = LB.at[s, t // 2, at]
            return pltpu.make_async_remote_copy(
                src_ref=WA.at[s, t // 2, y2, at] if from_wa else piece, dst_ref=piece,
                send_sem=ssem.at[base + 4 * ("x1", "x3", "zl").index(p) + t],
                recv_sem=rsem.at[base + t], device_id=dev[p], device_id_type=MESH)

        @pl.when(code == 0)
        def _():
            for a, b, zz in ((0, 2, 0), (1, 3, 2), (2, 0, 1), (3, 1, 3)):
                cp("x1", a, True).start()
                cp("x3", b, True).start()
                cp("zl", zz, True).start()
            for t in range(2):
                for q in range(4):
                    LB[s, t, q] = WA[s, t, y2, q]

        roles = {1: ((0, 1, 2, 3), {0: "x3", 1: "x3"}), 2: ((2, 3, 0, 1), {2: "x1", 3: "x1"}),
                 3: ((0, 2, 1, 3), {})}
        for n in range(4):
            yield
            for k, (order, onward) in roles.items():
                @pl.when(code == k)
                def _(order=order, onward=onward):
                    t = order[n]
                    cp("zl", t, False).wait_recv()
                    if t in onward:
                        cp(onward[t], t, False).start()
                    cp("zl", t, False).start()

            for k, order in ((4, (0, 2, 1, 3)), (5, (0, 1, 2, 3)), (6, (2, 3, 0, 1)), (7, (0, 2, 1, 3))):
                @pl.when(code == k)
                def _(order=order):
                    cp("zl", order[n], False).wait_recv()

            if beside is not None:
                beside(n)
            elif n == 3:
                arrived.append(s)

        def finish():
            @pl.when(code == 0)
            def _():
                for p in ("x1", "x3", "zl"):
                    for t in range(4):
                        cp(p, t, True).wait_send()

            for k, (order, onward) in roles.items():
                @pl.when(code == k)
                def _(onward=onward):
                    for t in range(4):
                        if t in onward:
                            cp(onward[t], t, False).wait_send()
                        cp("zl", t, False).wait_send()

        last.append(finish)

    def stream(s):
        yield from reduce_to_owner(s, 1)
        d = go(PT.at[s, 1, core, u1, u2, v1, v2], RG.at[s, zl, core, v1, v2], "zl")
        RG[s, zl, core, v1, v2] = PT[s, 0, core, u1, u2, v1, v2]
        yield
        d.wait_recv()

        def widen(*moves):
            ds_ = [go(RG.at[(s, every, core) + i + (every, lanes)],
                      RG.at[(s, every, core) + i + (every, lanes)], p) for i, lanes, p in moves]
            yield
            for d_ in ds_:
                d_.wait_recv()

        yield from widen(((v1, v2), LA, "z3"), ((v1, v2), LB_, "z1"))
        yield from widen(((v1, every), LA, "z1"), ((every, v2), LB_, "z3"))
        d = go(RG.at[s, :, core], RG.at[s, :, core], "core")
        yield
        d.wait_recv()
        acc = None
        for j in range(2):
            rh, rl = split(RG[s, j].reshape(64, 1024))
            lanes = pl.ds(j * 1024, 1024)
            t = mm3(rh, rl, DSh[0, :, lanes], DSh[1, :, lanes], ((1,), (1,)))
            acc = t if acc is None else acc + t
        WA[s, core, y, zh] = acc

        wz = Gather4(lambda h: WA.at[s, core, y, zh, 32 * h:32 * h + 32],
                     lambda i, h: WA.at[s, core, y, i, 32 * h:32 * h + 32], zh, zi1, zi3, "z1", "z3")
        yield
        wz.forward()
        yield
        wz.near()
        wz.far()
        wy = Gather4(lambda h: WA.at[s, core, y, 2 * h:2 * h + 2],
                     lambda i, h: WA.at[s, core, i, 2 * h:2 * h + 2], y, yi1, yi3, "y1", "y3")
        wc = [go(WA.at[s, core, y], WA.at[s, core, y], "core")]
        yield
        wy.forward()
        yield
        wy.near()
        for i in (yi1, yi3):
            wc.append(go(WA.at[s, core, i], WA.at[s, core, i], "core"))
        yield
        wy.far()
        wc.append(go(WA.at[s, core, yi2], WA.at[s, core, yi2], "core"))
        yield
        for d in wc:
            d.wait_recv()
        yield from spread(s, (None, beside)[s])

    def advance(*gens):
        for i in gens:
            next(i)

    def dsplit(q, _):
        for j in range(8):
            hi, lo = split(DS[q, j // 2, j % 2])
            lanes = pl.ds((j % 2) * 1024 + (j // 2) * 256, 256)
            DSh[0, pl.ds(al(q * 64, 64), 64), lanes] = hi
            DSh[1, pl.ds(al(q * 64, 64), 64), lanes] = lo
        return 0

    def more():
        k = 256 * len(w1)
        w1.append(swap_w(1, k, k + 256))

    both = (0, 1)
    convert(x)
    product(0, x, x, 0, KP, both, False)
    dy.forward()
    fx.forward()
    fx.near()
    more()
    for i in (xi1, xi3):
        convert(i)
        product(0, i, i, 0, KP, both, False)
    for d in w0:
        d.wait_recv()
    split_in(0, 0, KP)
    for i in (x, xi1, xi3):
        product(1, i, i, 0, KP, (0,), False)
    dy.near()
    dy.far()
    lax.fori_loop(0, 4, dsplit, 0)
    more()
    more()
    fx.far()
    convert(xi2)
    for h in range(2):
        product(h, xi2, xi2, 0, KP, (0,), False)
    early0, stream0 = reduce_to_owner(0, 0), stream(0)
    advance(early0, stream0)
    product(0, xi2, xi2, 0, KP, (1,), False)
    early1 = reduce_to_owner(1, 0)
    advance(early1)
    more()
    advance(early0, stream0)
    for j in range(4):
        w1[j].wait_recv()
    split_in(1, 0, 1024)
    product_all(1, 0, 1024, (1,), False)
    advance(early0, stream0, early1)
    for j in range(4, 6):
        w1[j].wait_recv()
    split_in(1, 1024, 1536)
    product_all(1, 1024, 1536, (1,), True)
    advance(early0, stream0, early1)
    for j in range(6, 8):
        w1[j].wait_recv()
        split_in(1, 256 * j, 256 * j + 256)
        product_all(1, 256 * j, 256 * j + 256, (1,), True)
    pending = [early0, stream0, early1, stream(1)]
    next(pending[-1])
    while pending:
        for i in list(pending):
            if next(i, "end") == "end":
                pending.remove(i)

    gram(1)
    for d in sends:
        d.wait_send()
    for end in last:
        end()
    assert nsem[0] <= NSEM


def body(f, wb, g, di):
    ft = f.T
    vm, dma = pltpu.VMEM, pltpu.SemaphoreType.DMA
    w, gram = pl.pallas_call(
        kernel,
        out_shape=(jax.ShapeDtypeStruct((64, 512), F32), jax.ShapeDtypeStruct((128, 512), F32)),
        in_specs=[pl.BlockSpec(memory_space=pl.ANY)] * 4,
        out_specs=(pl.BlockSpec(memory_space=pltpu.VMEM),) * 2,
        scratch_shapes=[
            vm((4, KD, 256), F32), vm((4, KP, 256), BF16), vm((4, KP, 256), BF16),
            vm((KP, 512), F32), vm((2, 256, KP), F32), vm((2, 256, KP), F32),
            vm((2, 2, 256, KP), BF16), vm((2, 2, 256, KP), BF16),
            vm((2, 2, 2, 2, 2, 2, 2, 8, 1024), F32), vm((2, 2, 2, 2, 2, 2, 8, 1024), F32),
            vm((2, 2, 2, 2, 2, 2, 8, 512), F32), vm((2, 2, 2, 2, 2, 8, 512), F32),
            vm((2, 2, 2, 2, 8, 512), F32), vm((2, 2, 2, 8, 512), F32),
            vm((2, 2, 2, 2, 2, 8, 1024), F32), vm((4, 4, 2, 64, 256), F32), vm((2, 256, 2048), BF16),
            vm((2, 2, 4, 4, 64, 256), F32), vm((2, 2, 4, 64, 256), F32), vm((4, 128, 128), F32),
            dma((NSEM,)), dma((NSEM,)), dma((10,)),
        ],
        compiler_params=pltpu.CompilerParams(collective_id=0, has_side_effects=True,
                                             vmem_limit_bytes=66_000_000),
        name="panel",
    )(ft, wb, g, di)
    return -w, gram * (1.0 / ROWS)


def solution(mesh):
    return jax.shard_map(
        body, mesh=mesh,
        in_specs=(P("pcol", "prow"), P("prow", "pcol"), P("prow", "pcol"), P("prow", "pcol")),
        out_specs=(P("prow", "pcol"), P("prow", "pcol")), check_vma=False)
```
